32 devices in a mesh: member: 2 (over y), slab: 4 (over z), chan: 2 (over x), mode: 2 (over core).
Axes of the slice: x: 2, y: 2, z: 4, core: 2. Of those that a mesh axis runs over, the one named last changes fastest.
Arguments:
- source_field: float32 [128, 1024, 1024], P(('member', 'chan'), 'slab', 'mode'), parts along dimension 0, may hold values from -6 to 6
- cotangent: float32 [128, 1024, 1024], P(('member', 'chan'), 'slab', 'mode'), parts along dimension 0, may hold values from -6 to 6
- spectral_weight: float32 [128, 64, 32, 2, 64], P(('member', 'chan'), None, 'mode', None, 'slab'), parts along dimension 0, may hold values from -12 to 12
- skip_gain: float32 [128], P(('member', 'chan')), parts along dimension 0, may hold values from 0.5 to 2
- channel_bias: float32 [128], P(('member', 'chan')), parts along dimension 0, may hold values from -0.5 to 0.5
- mode_limit: int32 [128, 2], P('member'), parts along dimension 0, may hold values from 16 to 32
- width_limit: int32 [128], P('member'), parts along dimension 0, may hold values from 32 to 64
Outputs:
- output: float32 [128, 1024, 1024], P(('member', 'chan'), 'slab', 'mode'), parts along dimension 0
- field_grad: float32 [128, 1024, 1024], P(('member', 'chan'), 'slab', 'mode'), parts along dimension 0
- spectral_grad: float32 [128, 64, 32, 2, 64], P(('member', 'chan'), None, 'mode', None, 'slab'), parts along dimension 0
- gate_grad: float32 [128], P(('member', 'chan')), parts along dimension 0
- bias_grad: float32 [128], P(('member', 'chan')), parts along dimension 0
The draws below stay inside these ranges and needn't reach their ends.
There are 2 independent parts, one for each index of `member`. The reference program is written for one: setup_inputs(seed, part) draws one part's arguments, and reference() takes and returns one part's arrays. A program takes and returns all parts, laid end to end along the dimension named above; each array names one. Nothing has to cross between parts.
Inputs may be any that keep to these rules, and one draw needn't show every extreme that they name: `mode_limit`: never more than 32. `width_limit`: never more than 64.
All inputs are finite; a program needn't handle non-finite values.
Results may differ from the reference program's by a relative error of at most 0.00018.
Values sent between devices are 32-bit elements; how exact they have to be, the bound alone decides.
A program may use at most 192 MiB of HBM per device.

```python
import math
import jax
import jax.numpy as jnp
from jax import lax

C = 64
H = 1024
W = 1024
M = 32
KX = 64


def plant(values, stream_key, low, high):
    longest = values.shape.index(max(values.shape))
    spots = []
    for shift in (0, 1):
        where = [jax.random.randint(jax.random.fold_in(stream_key, axis), (), 0, length) for axis, length in enumerate(values.shape)]
        where[longest] = (where[longest] + shift) % values.shape[longest]
        spots.append(tuple(where))
    return values.at[spots[0]].set(low).at[spots[1]].set(high)


def levels(rng, shape, split, least, largest):
    factor_of = 1.0
    for dim, parts in split:
        steps = jax.random.uniform(jax.random.fold_in(jax.random.fold_in(rng, 6), dim), (parts,), jnp.float32, least / len(split), largest / len(split))
        factor_of = factor_of * jnp.repeat(jnp.exp(steps), shape[dim] // parts).reshape((-1,) + (1,) * (len(shape) - 1 - dim))
    return factor_of


def scatter_about(rng, dims, width, most, pieces=(), kind=jnp.bfloat16):
    entries = jax.random.normal(rng, dims, jnp.float32) * width
    if len(pieces) > 0:
        entries = levels(rng, dims, pieces, -0.22, 0.18) * entries
    return jnp.clip(entries, min=-most, max=most).astype(kind)


def setup_inputs(seed: int = 0, part: int = 0) -> dict:
    seeds = jax.random.split(jax.random.key(seed), 8)
    part_keys = jax.random.split(jax.random.fold_in(seeds[7], part), 8)
    return {
        "source_field": scatter_about(part_keys[0], (C, H, W), 1.0, 6.0, ((0, 2), (1, 4), (2, 2)), jnp.float32),
        "cotangent": scatter_about(part_keys[1], (C, H, W), 1.0, 6.0, ((0, 2), (1, 4), (2, 2)), jnp.float32),
        "spectral_weight": scatter_about(part_keys[2], (C, C, M, 2, KX), 2.0, 12.0, ((0, 2), (2, 2), (4, 4)), jnp.float32),
        "skip_gain": jnp.clip(jnp.exp(math.log(2.0) - 1.3862944 * jax.random.uniform(part_keys[3], (C,), jnp.float32) ** levels(part_keys[3], (C,), ((0, 2),), -0.2, 0.2)), 0.5, 2.0),
        "channel_bias": jnp.clip(jax.random.uniform(part_keys[4], (C,), jnp.float32, -0.5, 0.5) * levels(part_keys[4], (C,), ((0, 2),), -0.4, 0.0), -0.5, 0.5),
        "mode_limit": plant(jax.random.randint(part_keys[5], (C, 2), M // 2, M + 1), jax.random.fold_in(part_keys[5], 1), M // 2, M).astype(jnp.int32),
        "width_limit": plant(jax.random.randint(part_keys[6], (C,), C // 2, C + 1), jax.random.fold_in(part_keys[6], 1), C // 2, C).astype(jnp.int32),
    }


precise = lax.Precision.HIGHEST

def column_table(extent, freq_count, first_cell, cell_count):
    cell_index = first_cell + jnp.arange(cell_count, dtype=jnp.int32)
    wave_index = jnp.arange(freq_count, dtype=jnp.int32)
    products = (cell_index[:, None] * wave_index[None, :] % extent).astype(jnp.float32)
    angles = products * (2.0 * math.pi / extent)
    return jnp.stack([jnp.cos(angles), -jnp.sin(angles)], axis=-1).reshape(cell_count, 2 * freq_count)

def row_tables(extent, freq_count, first_cell, cell_count):
    cell_index = first_cell + jnp.arange(cell_count, dtype=jnp.int32)
    column = jnp.arange(2 * freq_count, dtype=jnp.int32)
    wave_index = (column + jnp.where(column >= freq_count, extent - 2 * freq_count, 0)).astype(jnp.int32)
    products = (cell_index[:, None] * wave_index[None, :] % extent).astype(jnp.float32)
    angles = products * (2.0 * math.pi / extent)
    return (jnp.cos(angles), jnp.sin(angles))

def spectrum(values, column_tab, row_cos, row_sin):
    channels, row_count, col_count = values.shape
    freq_count = column_tab.shape[1] // 2
    halves = jnp.einsum('chw,wk->chk', values, column_tab, precision=precise).reshape(channels, row_count, freq_count, 2)
    real_part = halves[..., 0]
    imag_part = halves[..., 1]
    out_real = jnp.einsum('chy,hx->cyx', real_part, row_cos, precision=precise) + jnp.einsum('chy,hx->cyx', imag_part, row_sin, precision=precise)
    out_imag = jnp.einsum('chy,hx->cyx', imag_part, row_cos, precision=precise) - jnp.einsum('chy,hx->cyx', real_part, row_sin, precision=precise)
    return jnp.stack([out_real, out_imag], axis=2)

def synthesis(modes_in, column_tab, row_cos, row_sin):
    channels = modes_in.shape[0]
    real_part = modes_in[:, :, 0]
    imag_part = modes_in[:, :, 1]
    back_real = jnp.einsum('cyx,hx->cyh', real_part, row_cos, precision=precise) - jnp.einsum('cyx,hx->cyh', imag_part, row_sin, precision=precise)
    back_imag = jnp.einsum('cyx,hx->cyh', real_part, row_sin, precision=precise) + jnp.einsum('cyx,hx->cyh', imag_part, row_cos, precision=precise)
    joined = jnp.stack([back_real, back_imag], axis=2).reshape(channels, -1, row_cos.shape[0])
    return jnp.einsum('ckh,wk->chw', joined, column_tab, precision=precise)

def contract(spectra, weight):
    spec_real = spectra[:, :, 0]
    spec_imag = spectra[:, :, 1]
    weight_real = weight[:, :, :, 0]
    weight_imag = weight[:, :, :, 1]
    out_real = jnp.einsum('iyx,ioyx->oyx', spec_real, weight_real, precision=precise) - jnp.einsum('iyx,ioyx->oyx', spec_imag, weight_imag, precision=precise)
    out_imag = jnp.einsum('iyx,ioyx->oyx', spec_real, weight_imag, precision=precise) + jnp.einsum('iyx,ioyx->oyx', spec_imag, weight_real, precision=precise)
    return jnp.stack([out_real, out_imag], axis=2)

def contract_back(grads, weight):
    grad_real = grads[:, :, 0]
    grad_imag = grads[:, :, 1]
    weight_real = weight[:, :, :, 0]
    weight_imag = weight[:, :, :, 1]
    back_real = jnp.einsum('oyx,ioyx->iyx', grad_real, weight_real, precision=precise) + jnp.einsum('oyx,ioyx->iyx', grad_imag, weight_imag, precision=precise)
    back_imag = jnp.einsum('oyx,ioyx->iyx', grad_imag, weight_real, precision=precise) - jnp.einsum('oyx,ioyx->iyx', grad_real, weight_imag, precision=precise)
    return jnp.stack([back_real, back_imag], axis=2)

def outer_grad(spectra, grads):
    spec_real = spectra[:, :, 0]
    spec_imag = spectra[:, :, 1]
    grad_real = grads[:, :, 0]
    grad_imag = grads[:, :, 1]
    real_side = jnp.einsum('iyx,oyx->ioyx', spec_real, grad_real) + jnp.einsum('iyx,oyx->ioyx', spec_imag, grad_imag)
    imag_side = jnp.einsum('iyx,oyx->ioyx', spec_real, grad_imag) - jnp.einsum('iyx,oyx->ioyx', spec_imag, grad_real)
    return jnp.stack([real_side, imag_side], axis=3)

def mode_weights(limit_rows, col_freq, row_freq, kx_count, cells_total):
    keep_cols = col_freq[None, :] < limit_rows[:, 0:1]
    keep_rows = (row_freq[None, :] < limit_rows[:, 1:2]) | ((kx_count - row_freq)[None, :] < limit_rows[:, 1:2])
    scales = jnp.where(col_freq == 0, 1.0, 2.0).astype(jnp.float32) / cells_total
    joined = keep_cols[:, :, None] & keep_rows[:, None, :]
    return (joined.astype(jnp.float32) * scales[None, :, None])[:, :, None, :]

def read_mask(in_index, width_limit):
    return (in_index[:, None] < width_limit[None, :]).astype(jnp.float32)[:, :, None, None, None]

def reference(source_field, cotangent, spectral_weight, skip_gain, channel_bias, mode_limit, width_limit):
    channels, row_count, col_count = source_field.shape
    freq_count = spectral_weight.shape[2]
    kx_count = spectral_weight.shape[4]
    column_tab = column_table(col_count, freq_count, 0, col_count)
    row_cos, row_sin = row_tables(row_count, freq_count, 0, row_count)
    weights = mode_weights(mode_limit, jnp.arange(freq_count, dtype=jnp.int32), jnp.arange(kx_count, dtype=jnp.int32), kx_count, row_count * col_count)
    reads = read_mask(jnp.arange(channels, dtype=jnp.int32), width_limit)
    masked_weight = spectral_weight * reads
    spectra = spectrum(source_field, column_tab, row_cos, row_sin)
    out_modes = contract(spectra, masked_weight) * weights
    branch = synthesis(out_modes, column_tab, row_cos, row_sin)
    skip_scale = skip_gain[:, None, None]
    summed = branch + skip_scale * source_field + channel_bias[:, None, None]
    output, gelu_back = jax.vjp(jax.nn.gelu, summed)
    grad_sum = gelu_back(cotangent)[0]
    grad_modes = spectrum(grad_sum, column_tab, row_cos, row_sin) * weights
    spectral_grad = outer_grad(spectra, grad_modes) * reads
    field_grad = synthesis(contract_back(grad_modes, masked_weight), column_tab, row_cos, row_sin) + skip_scale * grad_sum
    gate_grad = lax.optimization_barrier(jnp.sum(grad_sum * source_field, axis=(1, 2)))
    bias_grad = lax.optimization_barrier(jnp.sum(grad_sum, axis=(1, 2)))
    return (output, field_grad, spectral_grad, gate_grad, bias_grad)
```

```python
import functools
import math

import jax
import jax.numpy as jnp
from jax import lax
from jax.experimental import pallas as pl
from jax.experimental.pallas import tpu as pltpu
from jax.sharding import PartitionSpec as P

LANES = 128
BIG = 60 * 1024 * 1024


def split_table(table):
    high = lax.reduce_precision(table, 8, 7)
    return high.astype(jnp.bfloat16), (table - high).astype(jnp.bfloat16)


def split_block(values):
    high = values.astype(jnp.bfloat16)
    return high, (values - high.astype(jnp.float32)).astype(jnp.bfloat16)


def dot_pair(left, right):
    left_high, left_low = left
    right_high, right_low = right
    mul = functools.partial(jnp.dot, preferred_element_type=jnp.float32)
    return mul(left_high, right_high) + mul(left_low, right_high) + mul(left_high, right_low)


def tables(extent, waves, first_cell, cell_count):
    cell_index = first_cell + jnp.arange(cell_count, dtype=jnp.int32)
    products = (cell_index[:, None] * waves[None, :] % extent).astype(jnp.float32)
    angles = products * (2.0 * math.pi / extent)
    return jnp.cos(angles), jnp.sin(angles)


def store_spectrum(values, col_pair, row_pair, out_ref):
    block, rows, cols = values.shape
    lines = dot_pair(split_block(values.reshape(block * rows, cols)), col_pair)
    kx = row_pair[0].shape[0] // 2
    half = lines.shape[1] // 2
    for c in range(block):
        mixed = dot_pair(row_pair, split_block(lines[c * rows : (c + 1) * rows]))
        sines = mixed[kx:]
        out_ref[c] = mixed[:kx] + jnp.concatenate([sines[:, half:], -sines[:, :half]], axis=1)


def synth(modes, row_pair, col_pair):
    half = modes.shape[1] // 2
    turned = jnp.concatenate([-modes[:, half:], modes[:, :half]], axis=1)
    stacked = jnp.concatenate([modes, turned], axis=0)
    lines = dot_pair(row_pair, split_block(stacked))
    return dot_pair(split_block(lines), col_pair)


def spectrum_kernel(x_ref, ch_ref, cl_ref, rh_ref, rl_ref, out_ref):
    store_spectrum(x_ref[...], (ch_ref[...], cl_ref[...]), (rh_ref[...], rl_ref[...]), out_ref)


def middle_kernel(
    x_ref, cot_ref, modes_ref, gain_ref, bias_ref, ch_ref, cl_ref, rh_ref, rl_ref,
    cth_ref, ctl_ref, ih_ref, il_ref, out_ref, grad_ref, spec_ref, sums_ref,
):
    block = x_ref.shape[0]
    row_back = (ih_ref[...], il_ref[...])
    col_back = (cth_ref[...], ctl_ref[...])
    scale = math.sqrt(2.0 / math.pi)
    for c in range(block):
        source = x_ref[c]
        gain = gain_ref[c]
        v = synth(modes_ref[c], row_back, col_back) + gain[:, :1] * source + bias_ref[c][:, :1]
        square = v * v
        t = jnp.tanh(scale * v * (1.0 + 0.044715 * square))
        half_up = 0.5 * (1.0 + t)
        out_ref[c] = v * half_up
        slope = half_up + 0.5 * v * (1.0 - t * t) * (scale * (1.0 + 3.0 * 0.044715 * square))
        grad = cot_ref[c] * slope
        grad_ref[c] = grad
        gate = jnp.sum(jnp.sum(grad * source, axis=0, keepdims=True), axis=1, keepdims=True)
        bias = jnp.sum(jnp.sum(grad, axis=0, keepdims=True), axis=1, keepdims=True)
        lane = lax.broadcasted_iota(jnp.int32, (1, LANES), 1)
        sums_ref[c] = jnp.where(lane == 0, gate, bias)
    store_spectrum(
        grad_ref[...], (ch_ref[...], cl_ref[...]), (rh_ref[...], rl_ref[...]), spec_ref
    )


def last_kernel(grad_ref, modes_ref, gain_ref, cth_ref, ctl_ref, ih_ref, il_ref, out_ref):
    for c in range(grad_ref.shape[0]):
        branch = synth(modes_ref[c], (ih_ref[...], il_ref[...]), (cth_ref[...], ctl_ref[...]))
        out_ref[c] = branch + gain_ref[c][:, :1] * grad_ref[c]


def contract_kernel(w_ref, spec_ref, limit_ref, out_ref):
    block, freqs, _, kx, outs = w_ref.shape
    first = lax.axis_index("chan") * (block * pl.num_programs(0)) + pl.program_id(0) * block

    @pl.when(pl.program_id(0) == 0)
    def _():
        out_ref[...] = jnp.zeros_like(out_ref)

    limit = limit_ref[...]
    for y in range(freqs):
        real = out_ref[y, 0]
        imag = out_ref[y, 1]
        for i in range(block):
            keep = first + i < limit
            spec = spec_ref[i]
            s_real = jnp.where(keep, spec[:, y : y + 1], 0.0)
            s_imag = jnp.where(keep, spec[:, freqs + y : freqs + y + 1], 0.0)
            w_real = w_ref[i, y, 0]
            w_imag = w_ref[i, y, 1]
            real = real + (s_real * w_real - s_imag * w_imag)
            imag = imag + (s_real * w_imag + s_imag * w_real)
        out_ref[y, 0] = real
        out_ref[y, 1] = imag


def back_kernel(w_ref, spec_ref, grads_ref, limit_ref, wgrad_ref, out_ref):
    block, freqs, _, kx, outs = w_ref.shape
    first = lax.axis_index("chan") * (block * pl.num_programs(0)) + pl.program_id(0) * block
    limit = limit_ref[...]
    lane = lax.broadcasted_iota(jnp.int32, (kx, 2 * freqs), 1)

    def one(i, carry):
        keep = first + i < limit
        spec = spec_ref[i]
        back = jnp.zeros((kx, 2 * freqs), jnp.float32)
        for y in range(freqs):
            g_real = jnp.where(keep, grads_ref[y, 0], 0.0)
            g_imag = jnp.where(keep, grads_ref[y, 1], 0.0)
            s_real = spec[:, y : y + 1]
            s_imag = spec[:, freqs + y : freqs + y + 1]
            wgrad_ref[i, y, 0] = s_real * g_real + s_imag * g_imag
            wgrad_ref[i, y, 1] = s_real * g_imag - s_imag * g_real
            w_real = w_ref[i, y, 0]
            w_imag = w_ref[i, y, 1]
            b_real = jnp.sum(g_real * w_real + g_imag * w_imag, axis=1, keepdims=True)
            b_imag = jnp.sum(g_imag * w_real - g_real * w_imag, axis=1, keepdims=True)
            back = jnp.where(lane == y, b_real, back)
            back = jnp.where(lane == freqs + y, b_imag, back)
        out_ref[i] = back
        return carry

    lax.fori_loop(0, block, one, 0)


def exchange_kernel(axes, sizes, gather, x_ref, out_ref, send_sem, recv_sem, own_sem):
    total = math.prod(sizes)
    me = lax.axis_index(axes[0])
    for axis, size in zip(axes[1:], sizes[1:]):
        me = me * size + lax.axis_index(axis)

    def place(index):
        coords = {}
        for axis, size in reversed(list(zip(axes, sizes))):
            coords[axis] = lax.rem(index, size)
            index = lax.div(index, size)
        return coords

    barrier = pltpu.get_barrier_semaphore()
    for step in range(1, total):
        pl.semaphore_signal(
            barrier, inc=1, device_id=place(lax.rem(me + step, total)),
            device_id_type=pl.DeviceIdType.MESH,
        )
    pl.semaphore_wait(barrier, total - 1)
    copies = []
    for step in range(1, total):
        peer = lax.rem(me + step, total)
        copy = pltpu.make_async_remote_copy(
            src_ref=x_ref if gather else x_ref.at[peer],
            dst_ref=out_ref.at[me],
            send_sem=send_sem.at[step],
            recv_sem=recv_sem.at[step],
            device_id=place(peer),
            device_id_type=pl.DeviceIdType.MESH,
        )
        copy.start()
        copies.append(copy)
    own = pltpu.make_async_copy(x_ref if gather else x_ref.at[me], out_ref.at[me], own_sem)
    own.start()
    own.wait()
    for copy in copies:
        copy.wait()


def exchange(values, axes, gather, ident):
    sizes = tuple(lax.axis_size(axis) for axis in axes)
    total = math.prod(sizes)
    piece = values.shape if gather else values.shape[1:]
    flat = values.reshape((-1, LANES) if gather else (total, -1, LANES))
    out = pl.pallas_call(
        functools.partial(exchange_kernel, axes, sizes, gather),
        out_shape=jax.ShapeDtypeStruct((total,) + flat.shape[-2:], jnp.float32),
        in_specs=[pl.BlockSpec(memory_space=pltpu.VMEM)],
        out_specs=pl.BlockSpec(memory_space=pltpu.VMEM),
        scratch_shapes=[
            pltpu.SemaphoreType.DMA((total,)),
            pltpu.SemaphoreType.DMA((total,)),
            pltpu.SemaphoreType.DMA,
        ],
        compiler_params=pltpu.CompilerParams(collective_id=ident, has_side_effects=True),
        name="exchange" + str(ident),
    )(flat)
    return out.reshape((total,) + piece)


def mode_weights(limit_rows, col_freq, row_freq, kx_count, cells_total):
    keep_cols = col_freq[None, :] < limit_rows[:, 0:1]
    keep_rows = (row_freq[None, :] < limit_rows[:, 1:2]) | (
        (kx_count - row_freq)[None, :] < limit_rows[:, 1:2]
    )
    scales = jnp.where(col_freq == 0, 1.0, 2.0).astype(jnp.float32) / cells_total
    joined = keep_rows[:, :, None] & keep_cols[:, None, :]
    return (joined.astype(jnp.float32) * scales[None, None, :])[:, :, None, :]


def local(
    source_field, cotangent, spectral_weight, skip_gain, channel_bias, mode_limit, width_limit
):
    channels, row_count, col_count = source_field.shape
    slabs = lax.axis_size("slab")
    modes = lax.axis_size("mode")
    chans = lax.axis_size("chan")
    slab_index = lax.axis_index("slab")
    mode_index = lax.axis_index("mode")
    chan_index = lax.axis_index("chan")
    outs = spectral_weight.shape[1]
    freqs = spectral_weight.shape[2]
    kx = spectral_weight.shape[4]
    all_freqs = freqs * modes
    all_kx = kx * slabs
    all_rows = row_count * slabs
    all_cols = col_count * modes

    col_waves = jnp.arange(all_freqs, dtype=jnp.int32)
    row_waves = jnp.arange(all_kx, dtype=jnp.int32)
    row_waves = row_waves + jnp.where(2 * row_waves >= all_kx, all_rows - all_kx, 0)
    col_cos, col_sin = tables(all_cols, col_waves, mode_index * col_count, col_count)
    row_cos, row_sin = tables(all_rows, row_waves, slab_index * row_count, row_count)
    col_tab = jnp.concatenate([col_cos, -col_sin], axis=1)
    row_tab = jnp.concatenate([row_cos, row_sin], axis=1)
    col_pair = split_table(col_tab)
    col_back = tuple(part.T for part in col_pair)
    row_back = split_table(row_tab)
    row_pair = tuple(part.T for part in row_back)

    block = 2
    cells = pl.BlockSpec((block, row_count, col_count), lambda c: (c, 0, 0))
    freq_cells = pl.BlockSpec((block, all_kx, 2 * all_freqs), lambda c: (c, 0, 0))
    per_channel = pl.BlockSpec((block, 1, LANES), lambda c: (c, 0, 0))
    field = jax.ShapeDtypeStruct(source_field.shape, jnp.float32)
    freq_field = jax.ShapeDtypeStruct((channels, all_kx, 2 * all_freqs), jnp.float32)
    params = pltpu.CompilerParams(
        dimension_semantics=("arbitrary",), vmem_limit_bytes=BIG
    )

    def whole(array):
        return pl.BlockSpec(array.shape, lambda c: (0,) * array.ndim)

    grid = (channels // block,)
    wide = lambda values: jnp.broadcast_to(values[:, None, None], (channels, 1, LANES))
    gain = wide(skip_gain)
    forward = col_pair + row_pair
    back = col_back + row_back

    def spread(partial, ident):
        cut = partial.reshape(channels, slabs, kx, 2, modes, freqs).transpose(1, 4, 0, 2, 3, 5)
        cut = cut.reshape(slabs * modes, channels, kx, 2 * freqs)
        return jnp.sum(exchange(cut, ("slab", "mode"), False, ident), axis=0)

    def joined(parts):
        parts = parts.reshape(slabs, modes, channels, kx, 2, freqs)
        return parts.transpose(2, 0, 3, 4, 1, 5).reshape(channels, all_kx, 2 * all_freqs)

    spectra = spread(
        pl.pallas_call(
            spectrum_kernel,
            grid=grid,
            in_specs=[cells] + [whole(t) for t in forward],
            out_specs=freq_cells,
            out_shape=freq_field,
            compiler_params=params,
            name="spectrum",
        )(source_field, *forward),
        0,
    )

    weight = spectral_weight.transpose(0, 2, 3, 4, 1)
    limit = width_limit.reshape(1, outs)
    in_block = 4
    w_spec = pl.BlockSpec((in_block, freqs, 2, kx, outs), lambda i: (i, 0, 0, 0, 0))
    s_spec = pl.BlockSpec((in_block, kx, 2 * freqs), lambda i: (i, 0, 0))
    mode_spec = pl.BlockSpec((freqs, 2, kx, outs), lambda i: (0, 0, 0, 0))
    limit_spec = pl.BlockSpec((1, outs), lambda i: (0, 0))
    partial_modes = pl.pallas_call(
        contract_kernel,
        grid=(channels // in_block,),
        in_specs=[w_spec, s_spec, limit_spec],
        out_specs=mode_spec,
        out_shape=jax.ShapeDtypeStruct((freqs, 2, kx, outs), jnp.float32),
        compiler_params=params,
        name="contract",
    )(weight, spectra, limit)
    halves = partial_modes.transpose(3, 2, 1, 0).reshape(chans, channels, kx, 2 * freqs)
    summed_modes = jnp.sum(exchange(halves, ("chan",), False, 1), axis=0)

    col_freq = mode_index * freqs + jnp.arange(freqs, dtype=jnp.int32)
    row_freq = slab_index * kx + jnp.arange(kx, dtype=jnp.int32)
    limit_rows = lax.dynamic_slice_in_dim(mode_limit, chan_index * channels, channels, 0)
    weights = mode_weights(limit_rows, col_freq, row_freq, all_kx, all_rows * all_cols)
    weights = jnp.broadcast_to(weights, (channels, kx, 2, freqs)).reshape(
        channels, kx, 2 * freqs
    )
    out_modes = joined(exchange(summed_modes * weights, ("slab", "mode"), True, 2))

    output, grad_sum, grad_partial, sums = pl.pallas_call(
        middle_kernel,
        grid=grid,
        in_specs=[cells, cells, freq_cells, per_channel, per_channel]
        + [whole(t) for t in forward + back],
        out_specs=[cells, cells, freq_cells, per_channel],
        out_shape=[
            field,
            field,
            freq_field,
            jax.ShapeDtypeStruct((channels, 1, LANES), jnp.float32),
        ],
        compiler_params=params,
        name="middle",
    )(source_field, cotangent, out_modes, gain, wide(channel_bias), *forward, *back)

    grad_modes = spread(grad_partial, 3) * weights
    all_grads = exchange(grad_modes, ("chan",), True, 4)
    all_grads = all_grads.reshape(outs, kx, 2, freqs).transpose(3, 2, 1, 0)
    weight_grad, back_modes = pl.pallas_call(
        back_kernel,
        grid=(channels // in_block,),
        in_specs=[w_spec, s_spec, mode_spec, limit_spec],
        out_specs=[w_spec, s_spec],
        out_shape=[
            jax.ShapeDtypeStruct(weight.shape, jnp.float32),
            jax.ShapeDtypeStruct(spectra.shape, jnp.float32),
        ],
        compiler_params=params,
        name="back",
    )(weight, spectra, all_grads, limit)
    spectral_grad = weight_grad.transpose(0, 4, 1, 2, 3)

    sent = back_modes.size // LANES
    row_sums = sums[:, 0, :2].T.reshape(-1)
    extra = -(-row_sums.size // (8 * LANES)) * 8
    row_sums = jnp.pad(row_sums, (0, extra * LANES - row_sums.size)).reshape(extra, LANES)
    packed = jnp.concatenate([back_modes.reshape(sent, LANES), row_sums], axis=0)
    parts = exchange(packed, ("slab", "mode"), True, 5)
    field_modes = joined(parts[:, :sent])
    totals = jnp.sum(parts[:, sent:], axis=0).reshape(-1)
    gate_grad = totals[:channels]
    bias_grad = totals[channels : 2 * channels]
    field_grad = pl.pallas_call(
        last_kernel,
        grid=grid,
        in_specs=[cells, freq_cells, per_channel] + [whole(t) for t in back],
        out_specs=cells,
        out_shape=field,
        compiler_params=params,
        name="last",
    )(grad_sum, field_modes, gain, *back)
    return (output, field_grad, spectral_grad, gate_grad, bias_grad)


def solution(mesh):
    in_specs = (
        P(("member", "chan"), "slab", "mode"),
        P(("member", "chan"), "slab", "mode"),
        P(("member", "chan"), None, "mode", None, "slab"),
        P(("member", "chan")),
        P(("member", "chan")),
        P("member", None),
        P("member"),
    )
    out_specs = (
        P(("member", "chan"), "slab", "mode"),
        P(("member", "chan"), "slab", "mode"),
        P(("member", "chan"), None, "mode", None, "slab"),
        P(("member", "chan")),
        P(("member", "chan")),
    )
    return jax.shard_map(local, mesh=mesh, in_specs=in_specs, out_specs=out_specs, check_vma=False)
```

```python
import functools
import math

import jax
import jax.numpy as jnp
from jax import lax
from jax.experimental import pallas as pl
from jax.experimental.pallas import tpu as pltpu
from jax.sharding import PartitionSpec as P

LANES = 128
BIG = 60 * 1024 * 1024


def split_table(table):
    high = lax.reduce_precision(table, 8, 7)
    return high.astype(jnp.bfloat16), (table - high).astype(jnp.bfloat16)


def split_block(values):
    high = values.astype(jnp.bfloat16)
    return high, (values - high.astype(jnp.float32)).astype(jnp.bfloat16)


def dot_pair(left, right):
    left_high, left_low = left
    right_high, right_low = right
    mul = functools.partial(jnp.dot, preferred_element_type=jnp.float32)
    return mul(left_high, right_high) + mul(left_low, right_high) + mul(left_high, right_low)


def tables(extent, waves, first_cell, cell_count):
    cell_index = first_cell + jnp.arange(cell_count, dtype=jnp.int32)
    products = (cell_index[:, None] * waves[None, :] % extent).astype(jnp.float32)
    angles = products * (2.0 * math.pi / extent)
    return jnp.cos(angles), jnp.sin(angles)


def store_spectrum(values, col_pair, row_pair, out_ref):
    block, rows, cols = values.shape
    lines = dot_pair(split_block(values.reshape(block * rows, cols)), col_pair)
    all_kx = row_pair[0].shape[0] // 2
    kx, lanes = out_ref.shape[2:]
    span = lanes // block
    mode_count = lines.shape[1] // span
    slabs = out_ref.shape[0] // mode_count
    done = []
    for c in range(block):
        mixed = dot_pair(row_pair, split_block(lines[c * rows : (c + 1) * rows]))
        done.append(mixed[:all_kx] - turn(mixed[all_kx:], span))
    for m in range(mode_count):
        packed = jnp.concatenate([one[:, m * span : (m + 1) * span] for one in done], axis=1)
        for s in range(slabs):
            out_ref[m * slabs + s, 0] = packed[s * kx : (s + 1) * kx]


def turn(values, span):
    half = span // 2
    pieces = []
    for first in range(0, values.shape[1], span):
        pieces.append(-values[:, first + half : first + span])
        pieces.append(values[:, first : first + half])
    return jnp.concatenate(pieces, axis=1)


def all_modes(modes_ref, mode_count, c, block):
    span = modes_ref.shape[3] // block
    slabs = modes_ref.shape[0] // mode_count
    columns = []
    for m in range(mode_count):
        stack = [modes_ref[m * slabs + s, 0] for s in range(slabs)]
        columns.append(jnp.concatenate(stack, axis=0)[:, c * span : (c + 1) * span])
    return jnp.concatenate(columns, axis=1), span


def synth(modes_and_span, row_pair, col_pair):
    modes, span = modes_and_span
    stacked = jnp.concatenate([modes, turn(modes, span)], axis=0)
    lines = dot_pair(row_pair, split_block(stacked))
    return dot_pair(split_block(lines), col_pair)


def spectrum_kernel(x_ref, ch_ref, cl_ref, rh_ref, rl_ref, out_ref):
    store_spectrum(x_ref[...], (ch_ref[...], cl_ref[...]), (rh_ref[...], rl_ref[...]), out_ref)


def middle_kernel(
    mode_count, x_ref, cot_ref, modes_ref, gain_ref, bias_ref, ch_ref, cl_ref, rh_ref, rl_ref,
    cth_ref, ctl_ref, ih_ref, il_ref, out_ref, grad_ref, spec_ref, sums_ref,
):
    block = x_ref.shape[0]
    row_back = (ih_ref[...], il_ref[...])
    col_back = (cth_ref[...], ctl_ref[...])
    scale = math.sqrt(2.0 / math.pi)
    for c in range(block):
        source = x_ref[c]
        gain = gain_ref[c]
        v = synth(all_modes(modes_ref, mode_count, c, block), row_back, col_back) + gain[:, :1] * source + bias_ref[c][:, :1]
        square = v * v
        t = jnp.tanh(scale * v * (1.0 + 0.044715 * square))
        half_up = 0.5 * (1.0 + t)
        out_ref[c] = v * half_up
        slope = half_up + 0.5 * v * (1.0 - t * t) * (scale * (1.0 + 3.0 * 0.044715 * square))
        grad = cot_ref[c] * slope
        grad_ref[c] = grad
        gate = jnp.sum(jnp.sum(grad * source, axis=0, keepdims=True), axis=1, keepdims=True)
        bias = jnp.sum(jnp.sum(grad, axis=0, keepdims=True), axis=1, keepdims=True)
        lane = lax.broadcasted_iota(jnp.int32, (1, LANES), 1)
        sums_ref[c] = jnp.where(lane == 0, gate, bias)
    store_spectrum(
        grad_ref[...], (ch_ref[...], cl_ref[...]), (rh_ref[...], rl_ref[...]), spec_ref
    )


def last_kernel(mode_count, grad_ref, modes_ref, gain_ref, cth_ref, ctl_ref, ih_ref, il_ref, out_ref):
    block = grad_ref.shape[0]
    for c in range(block):
        modes = all_modes(modes_ref, mode_count, c, block)
        branch = synth(modes, (ih_ref[...], il_ref[...]), (cth_ref[...], ctl_ref[...]))
        out_ref[c] = branch + gain_ref[c][:, :1] * grad_ref[c]


def contract_kernel(w_ref, spec_ref, limit_ref, out_ref):
    block, freqs, _, kx, outs = w_ref.shape
    first = lax.axis_index("chan") * (block * pl.num_programs(0)) + pl.program_id(0) * block

    @pl.when(pl.program_id(0) == 0)
    def _():
        out_ref[...] = jnp.zeros_like(out_ref)

    limit = limit_ref[...]
    for y in range(freqs):
        real = out_ref[y, 0]
        imag = out_ref[y, 1]
        for i in range(block):
            keep = first + i < limit
            spec = spec_ref[0]
            at = 2 * freqs * i + y
            s_real = jnp.where(keep, spec[:, at : at + 1], 0.0)
            s_imag = jnp.where(keep, spec[:, freqs + at : freqs + at + 1], 0.0)
            w_real = w_ref[i, y, 0]
            w_imag = w_ref[i, y, 1]
            real = real + (s_real * w_real - s_imag * w_imag)
            imag = imag + (s_real * w_imag + s_imag * w_real)
        out_ref[y, 0] = real
        out_ref[y, 1] = imag


def back_kernel(w_ref, spec_ref, grads_ref, limit_ref, wgrad_ref, out_ref):
    block, freqs, _, kx, outs = w_ref.shape
    first = lax.axis_index("chan") * (block * pl.num_programs(0)) + pl.program_id(0) * block
    limit = limit_ref[...]
    lane = lax.broadcasted_iota(jnp.int32, out_ref.shape[1:], 1)
    spec = spec_ref[0]
    back = jnp.zeros(out_ref.shape[1:], jnp.float32)
    for i in range(block):
        keep = first + i < limit
        for y in range(freqs):
            at = 2 * freqs * i + y
            g_real = jnp.where(keep, grads_ref[y, 0], 0.0)
            g_imag = jnp.where(keep, grads_ref[y, 1], 0.0)
            s_real = spec[:, at : at + 1]
            s_imag = spec[:, freqs + at : freqs + at + 1]
            wgrad_ref[i, y, 0] = s_real * g_real + s_imag * g_imag
            wgrad_ref[i, y, 1] = s_real * g_imag - s_imag * g_real
            w_real = w_ref[i, y, 0]
            w_imag = w_ref[i, y, 1]
            b_real = jnp.sum(g_real * w_real + g_imag * w_imag, axis=1, keepdims=True)
            b_imag = jnp.sum(g_imag * w_real - g_real * w_imag, axis=1, keepdims=True)
            back = jnp.where(lane == at, b_real, back)
            back = jnp.where(lane == freqs + at, b_imag, back)
    out_ref[0] = back


def exchange_kernel(axes, sizes, gather, x_ref, out_ref, send_sem, recv_sem, own_sem):
    total = math.prod(sizes)
    me = lax.axis_index(axes[0])
    for axis, size in zip(axes[1:], sizes[1:]):
        me = me * size + lax.axis_index(axis)

    def place(index):
        coords = {}
        for axis, size in reversed(list(zip(axes, sizes))):
            coords[axis] = lax.rem(index, size)
            index = lax.div(index, size)
        return coords

    barrier = pltpu.get_barrier_semaphore()
    for step in range(1, total):
        pl.semaphore_signal(
            barrier, inc=1, device_id=place(lax.rem(me + step, total)),
            device_id_type=pl.DeviceIdType.MESH,
        )
    pl.semaphore_wait(barrier, total - 1)
    copies = []
    for step in range(1, total):
        peer = lax.rem(me + step, total)
        copy = pltpu.make_async_remote_copy(
            src_ref=x_ref if gather else x_ref.at[peer],
            dst_ref=out_ref.at[me],
            send_sem=send_sem.at[step],
            recv_sem=recv_sem.at[step],
            device_id=place(peer),
            device_id_type=pl.DeviceIdType.MESH,
        )
        copy.start()
        copies.append(copy)
    own = pltpu.make_async_copy(x_ref if gather else x_ref.at[me], out_ref.at[me], own_sem)
    own.start()
    own.wait()
    for copy in copies:
        copy.wait()


def exchange(values, axes, gather, ident):
    sizes = tuple(lax.axis_size(axis) for axis in axes)
    total = math.prod(sizes)
    piece = values.shape if gather else values.shape[1:]
    flat = values.reshape((-1, LANES) if gather else (total, -1, LANES))
    out = pl.pallas_call(
        functools.partial(exchange_kernel, axes, sizes, gather),
        out_shape=jax.ShapeDtypeStruct((total,) + flat.shape[-2:], jnp.float32),
        in_specs=[pl.BlockSpec(memory_space=pltpu.VMEM)],
        out_specs=pl.BlockSpec(memory_space=pltpu.VMEM),
        scratch_shapes=[
            pltpu.SemaphoreType.DMA((total,)),
            pltpu.SemaphoreType.DMA((total,)),
            pltpu.SemaphoreType.DMA,
        ],
        compiler_params=pltpu.CompilerParams(collective_id=ident, has_side_effects=True),
        name="exchange" + str(ident),
    )(flat)
    return out.reshape((total,) + piece)


def mode_weights(limit_rows, col_freq, row_freq, kx_count, cells_total):
    keep_cols = col_freq[None, :] < limit_rows[:, 0:1]
    keep_rows = (row_freq[None, :] < limit_rows[:, 1:2]) | (
        (kx_count - row_freq)[None, :] < limit_rows[:, 1:2]
    )
    scales = jnp.where(col_freq == 0, 1.0, 2.0).astype(jnp.float32) / cells_total
    joined = keep_rows[:, :, None] & keep_cols[:, None, :]
    return (joined.astype(jnp.float32) * scales[None, None, :])[:, :, None, :]


def local(
    source_field, cotangent, spectral_weight, skip_gain, channel_bias, mode_limit, width_limit
):
    channels, row_count, col_count = source_field.shape
    slabs = lax.axis_size("slab")
    modes = lax.axis_size("mode")
    chans = lax.axis_size("chan")
    slab_index = lax.axis_index("slab")
    mode_index = lax.axis_index("mode")
    chan_index = lax.axis_index("chan")
    outs = spectral_weight.shape[1]
    freqs = spectral_weight.shape[2]
    kx = spectral_weight.shape[4]
    all_freqs = freqs * modes
    all_kx = kx * slabs
    all_rows = row_count * slabs
    all_cols = col_count * modes

    col_waves = jnp.arange(all_freqs, dtype=jnp.int32)
    row_waves = jnp.arange(all_kx, dtype=jnp.int32)
    row_waves = row_waves + jnp.where(2 * row_waves >= all_kx, all_rows - all_kx, 0)
    col_cos, col_sin = tables(all_cols, col_waves, mode_index * col_count, col_count)
    row_cos, row_sin = tables(all_rows, row_waves, slab_index * row_count, row_count)
    col_tab = jnp.stack(
        [col_cos.reshape(-1, modes, freqs), -col_sin.reshape(-1, modes, freqs)], axis=2
    ).reshape(col_count, 2 * all_freqs)
    row_tab = jnp.concatenate([row_cos, row_sin], axis=1)
    col_pair = split_table(col_tab)
    col_back = tuple(part.T for part in col_pair)
    row_back = split_table(row_tab)
    row_pair = tuple(part.T for part in row_back)

    block = LANES // (2 * freqs)
    groups = channels // block
    owners = slabs * modes
    cells = pl.BlockSpec((block, row_count, col_count), lambda c: (c, 0, 0))
    freq_cells = pl.BlockSpec((owners, 1, kx, LANES), lambda c: (0, c, 0, 0))
    per_channel = pl.BlockSpec((block, 1, LANES), lambda c: (c, 0, 0))
    field = jax.ShapeDtypeStruct(source_field.shape, jnp.float32)
    freq_field = jax.ShapeDtypeStruct((owners, groups, kx, LANES), jnp.float32)
    params = pltpu.CompilerParams(
        dimension_semantics=("arbitrary",), vmem_limit_bytes=BIG
    )

    def whole(array):
        return pl.BlockSpec(array.shape, lambda c: (0,) * array.ndim)

    grid = (channels // block,)
    wide = lambda values: jnp.broadcast_to(values[:, None, None], (channels, 1, LANES))
    gain = wide(skip_gain)
    forward = col_pair + row_pair
    back = col_back + row_back

    def spread(partial, ident):
        half = exchange(partial.reshape(modes, -1, LANES), ("mode",), False, ident)
        half = jnp.sum(half, axis=0).reshape(slabs, -1, LANES)
        return jnp.sum(exchange(half, ("slab",), False, ident + 1), axis=0).reshape(
            groups, kx, LANES
        )

    def joined(piece, ident):
        half = exchange(piece, ("slab",), True, ident)
        return exchange(half, ("mode",), True, ident + 1).reshape((owners,) + piece.shape)

    spectra = spread(
        pl.pallas_call(
            spectrum_kernel,
            grid=grid,
            in_specs=[cells] + [whole(t) for t in forward],
            out_specs=freq_cells,
            out_shape=freq_field,
            compiler_params=params,
            name="spectrum",
        )(source_field, *forward),
        0,
    )

    weight = spectral_weight.transpose(0, 2, 3, 4, 1)
    limit = width_limit.reshape(1, outs)
    in_block = block
    w_spec = pl.BlockSpec((in_block, freqs, 2, kx, outs), lambda i: (i, 0, 0, 0, 0))
    s_spec = pl.BlockSpec((1, kx, LANES), lambda i: (i, 0, 0))
    mode_spec = pl.BlockSpec((freqs, 2, kx, outs), lambda i: (0, 0, 0, 0))
    limit_spec = pl.BlockSpec((1, outs), lambda i: (0, 0))
    partial_modes = pl.pallas_call(
        contract_kernel,
        grid=(channels // in_block,),
        in_specs=[w_spec, s_spec, limit_spec],
        out_specs=mode_spec,
        out_shape=jax.ShapeDtypeStruct((freqs, 2, kx, outs), jnp.float32),
        compiler_params=params,
        name="contract",
    )(weight, spectra, limit)
    halves = partial_modes.reshape(freqs, 2, kx, chans, groups, block)
    halves = halves.transpose(3, 4, 2, 5, 1, 0).reshape(chans, groups, kx, LANES)
    summed_modes = jnp.sum(exchange(halves, ("chan",), False, 2), axis=0)

    col_freq = mode_index * freqs + jnp.arange(freqs, dtype=jnp.int32)
    row_freq = slab_index * kx + jnp.arange(kx, dtype=jnp.int32)
    limit_rows = lax.dynamic_slice_in_dim(mode_limit, chan_index * channels, channels, 0)
    weights = mode_weights(limit_rows, col_freq, row_freq, all_kx, all_rows * all_cols)
    weights = jnp.broadcast_to(weights, (channels, kx, 2, freqs))
    weights = weights.reshape(groups, block, kx, 2 * freqs).transpose(0, 2, 1, 3)
    weights = weights.reshape(groups, kx, LANES)
    out_modes = joined(summed_modes * weights, 3)

    output, grad_sum, grad_partial, sums = pl.pallas_call(
        functools.partial(middle_kernel, modes),
        grid=grid,
        in_specs=[cells, cells, freq_cells, per_channel, per_channel]
        + [whole(t) for t in forward + back],
        out_specs=[cells, cells, freq_cells, per_channel],
        out_shape=[
            field,
            field,
            freq_field,
            jax.ShapeDtypeStruct((channels, 1, LANES), jnp.float32),
        ],
        compiler_params=params,
        name="middle",
    )(source_field, cotangent, out_modes, gain, wide(channel_bias), *forward, *back)

    grad_modes = spread(grad_partial, 5) * weights
    all_grads = exchange(grad_modes, ("chan",), True, 7)
    all_grads = all_grads.reshape(chans, groups, kx, block, 2, freqs)
    all_grads = all_grads.transpose(5, 4, 2, 0, 1, 3).reshape(freqs, 2, kx, outs)
    weight_grad, back_modes = pl.pallas_call(
        back_kernel,
        grid=(channels // in_block,),
        in_specs=[w_spec, s_spec, mode_spec, limit_spec],
        out_specs=[w_spec, s_spec],
        out_shape=[
            jax.ShapeDtypeStruct(weight.shape, jnp.float32),
            jax.ShapeDtypeStruct(spectra.shape, jnp.float32),
        ],
        compiler_params=params,
        name="back",
    )(weight, spectra, all_grads, limit)
    spectral_grad = weight_grad.transpose(0, 4, 1, 2, 3)

    sent = back_modes.size // LANES
    row_sums = sums[:, 0, :2].T.reshape(-1)
    extra = -(-row_sums.size // (8 * LANES)) * 8
    row_sums = jnp.pad(row_sums, (0, extra * LANES - row_sums.size)).reshape(extra, LANES)
    packed = jnp.concatenate([back_modes.reshape(sent, LANES), row_sums], axis=0)
    parts = joined(packed, 8)
    field_modes = parts[:, :sent].reshape(owners, groups, kx, LANES)
    totals = jnp.sum(parts[:, sent:], axis=0).reshape(-1)
    gate_grad = totals[:channels]
    bias_grad = totals[channels : 2 * channels]
    field_grad = pl.pallas_call(
        functools.partial(last_kernel, modes),
        grid=grid,
        in_specs=[cells, freq_cells, per_channel] + [whole(t) for t in back],
        out_specs=cells,
        out_shape=field,
        compiler_params=params,
        name="last",
    )(grad_sum, field_modes, gain, *back)
    return (output, field_grad, spectral_grad, gate_grad, bias_grad)


def solution(mesh):
    in_specs = (
        P(("member", "chan"), "slab", "mode"),
        P(("member", "chan"), "slab", "mode"),
        P(("member", "chan"), None, "mode", None, "slab"),
        P(("member", "chan")),
        P(("member", "chan")),
        P("member", None),
        P("member"),
    )
    out_specs = (
        P(("member", "chan"), "slab", "mode"),
        P(("member", "chan"), "slab", "mode"),
        P(("member", "chan"), None, "mode", None, "slab"),
        P(("member", "chan")),
        P(("member", "chan")),
    )
    return jax.shard_map(local, mesh=mesh, in_specs=in_specs, out_specs=out_specs, check_vma=False)
```
